32 devices in a mesh: orb: 32 (over z, y, x, core).
Axes of the slice: x: 2, y: 2, z: 4, core: 2. Of those that a mesh axis runs over, the one named last changes fastest.
Arguments:
- orbitals: float32 [64, 48, 64, 128], P('orb'), may hold values from -6 to 6
- pair_list: int32 [32, 6, 2], P('orb'), may hold values from 0 to 63, as said below
- pair_count: int32 [32], P('orb'), may hold values from 1 to 6, 64 in all
- box_offset: int32 [64, 3], replicated, may hold values from 0 to 24
Outputs:
- exchange: float32 [64, 48, 64, 128], P('orb')
The draws below stay inside these ranges and needn't reach their ends.
Inputs may be any that keep to these rules, and one draw needn't show every extreme that they name: `pair_list`: every orbital named in row d is owned by a device d - 1 to d + 1; the two orbitals of a pair differ; slot 0 of every row pairs with an orbital of a device exactly 1 away. `pair_count`: they sum to 64.
All inputs are finite; a program needn't handle non-finite values. No bound on the sum of `pair_count` on one device may be relied on, other than what follows from the above.
Results may differ from the reference program's by a relative error of at most 0.0003.
Values sent between devices are 32-bit elements; how exact they have to be, the bound alone decides.
A program may use at most 128 MiB of HBM per device.

```python
import math
import jax
import jax.numpy as jnp
import numpy as np
from jax import lax

BOX_X = 48
BOX_Y = 64
BOX_Z = 128
ORB_DEV = 2
SLOTS = 6
REACH = 1
SWEEPS = 12
RANKS = 32
ORBS = 64


def draw_pair_list(key, part):
    subkeys = jax.random.split(jax.random.fold_in(key, 7), 4)
    device = jnp.arange(RANKS, dtype=jnp.int32)[:, None]
    lead_shift = jax.random.randint(subkeys[0], (RANKS, SLOTS), -REACH, REACH + 1)
    lead_device = jnp.clip(device + lead_shift, 0, RANKS - 1)
    partner_shift = jax.random.randint(subkeys[1], (RANKS, SLOTS), -REACH, REACH + 1)
    boundary = jnp.where(device + REACH < RANKS, REACH, -REACH)
    slot_zero = jnp.arange(SLOTS, dtype=jnp.int32)[None, :] == 0
    partner_shift = jnp.where(slot_zero, boundary, partner_shift)
    partner_device = jnp.clip(device + partner_shift, 0, RANKS - 1)
    leading = lead_device * ORB_DEV + jax.random.randint(subkeys[2], (RANKS, SLOTS), 0, ORB_DEV)
    partner_local = jax.random.randint(subkeys[3], (RANKS, SLOTS), 0, ORB_DEV)
    partner = partner_device * ORB_DEV + partner_local
    partner = jnp.where(partner == leading, partner_device * ORB_DEV + (partner_local + 1) % ORB_DEV, partner)
    return jnp.stack([leading, partner], -1).astype(jnp.int32)


def touch_ends(array, key, low, largest):
    longest = array.shape.index(max(array.shape))
    spots = []
    for shift in (0, 1):
        where = [jax.random.randint(jax.random.fold_in(key, axis), (), 0, length) for axis, length in enumerate(array.shape)]
        where[longest] = (where[longest] + shift) % array.shape[longest]
        spots.append(tuple(where))
    return array.at[spots[0]].set(low).at[spots[1]].set(largest)


def block_scale(stream_key, shape, shards, least, top_value):
    def one(dim, blocks):
        draws = jax.random.uniform(jax.random.fold_in(jax.random.fold_in(stream_key, 6), dim), (blocks,), jnp.float32, least / len(shards), top_value / len(shards))
        return jnp.repeat(jnp.exp(draws), shape[dim] // blocks).reshape((-1,) + (1,) * (len(shape) - dim - 1))

    loudness = one(*shards[0])
    for cut in shards[1:]:
        loudness = loudness * one(*cut)
    return loudness


def profile(amount, total, bound, slope):
    loads = [(1 << 20) // math.isqrt(grade ** slope) + 1 for grade in range(2, amount + 1)]
    rest, holding = total - bound - (amount - 1), [1] * (amount - 1)
    while rest > 0:
        movable = [i for i in range(amount - 1) if holding[i] < bound]
        whole, left = sum([loads[i] for i in movable]), rest
        for i in movable:
            more = min(bound - holding[i], max(1, left * loads[i] // whole), rest)
            holding[i] = holding[i] + more
            rest = rest - more
    return np.array([bound] + holding)


def uneven_parts(rng, number_of, total, bound, skew):
    if number_of == 2:
        one = jax.random.randint(rng, (), max(1, total - bound), min(bound, total - 1) + 1)
        return jnp.stack([one, total - one])
    sizes = jnp.asarray(profile(number_of, total, bound, skew), jnp.int32)
    couples = (number_of - 1) // 2
    donor, receiver = sizes[1:1 + 2 * couples:2], sizes[2:2 + 2 * couples:2]
    slack = jnp.minimum(donor - 1, bound - receiver)
    shifted = jax.random.randint(jax.random.fold_in(rng, 1), (couples,), 0, 1 << 20) % (slack + 1)
    sizes = sizes.at[1:1 + 2 * couples:2].set(donor - shifted).at[2:2 + 2 * couples:2].set(receiver + shifted)
    return sizes[jax.random.permutation(jax.random.fold_in(rng, 2), number_of)]


def normal_values(key, extent, deviation, bound, cuts=(), kind=jnp.bfloat16):
    drawn = deviation * jax.random.normal(key, extent, jnp.float32)
    if cuts:
        drawn = drawn * block_scale(key, extent, cuts, -0.22, 0.18)
    return jnp.clip(drawn, -bound, bound).astype(kind)


def setup_inputs(seed: int = 0) -> dict:
    streams_of = jax.random.split(jax.random.key(seed), 5)
    return {
        "orbitals": normal_values(streams_of[0], (ORBS, BOX_X, BOX_Y, BOX_Z), 1.0, 6.0, ((0, 32),), jnp.float32),
        "pair_list": draw_pair_list(jax.random.fold_in(streams_of[4], 71), 0),
        "pair_count": uneven_parts(streams_of[2], RANKS, ORBS, SLOTS, 2).astype(jnp.int32),
        "box_offset": touch_ends(jax.random.randint(streams_of[3], (ORBS, 3), 0, BOX_X // 2 + 1), jax.random.fold_in(streams_of[3], 1), 0, (BOX_X // 2 + 1) - 1).astype(jnp.int32),
    }


def jacobi_solve(source_term):
    def sweep(sweep_index, potential):
        padded = jnp.pad(potential, 1)
        beside = padded[2:, 1:-1, 1:-1] + padded[:-2, 1:-1, 1:-1]
        beside = beside + padded[1:-1, 2:, 1:-1] + padded[1:-1, :-2, 1:-1]
        beside = beside + padded[1:-1, 1:-1, 2:] + padded[1:-1, 1:-1, :-2]
        return (beside + source_term) / 6.0
    return lax.fori_loop(0, SWEEPS, sweep, jnp.zeros_like(source_term))


def displaced(values_in, corner):
    margin = BOX_X // 2
    padded = jnp.pad(values_in, margin)
    return lax.dynamic_slice(padded, (corner[0], corner[1], corner[2]), values_in.shape)


def pair_terms(leading_box, partner_box, offset_gap):
    margin = BOX_X // 2
    partner = displaced(partner_box, margin - offset_gap)
    potential = jacobi_solve(leading_box * partner)
    own_term = potential * partner
    back_term = displaced(potential * leading_box, margin + offset_gap)
    return own_term, back_term


def reference(orbitals, pair_list, pair_count, box_offset):
    flat_pairs = pair_list.reshape(RANKS * SLOTS, 2)
    owners = jnp.repeat(jnp.arange(RANKS, dtype=jnp.int32), SLOTS)
    slot_index = jnp.tile(jnp.arange(SLOTS, dtype=jnp.int32), RANKS)
    live_mask = slot_index < pair_count[owners]

    def visit_pair(accum, element):
        pair_entry, is_live = element

        def add_pair(current):
            leading, partner = pair_entry[0], pair_entry[1]
            offset_gap = box_offset[partner] - box_offset[leading]
            own_term, back_term = pair_terms(orbitals[leading], orbitals[partner], offset_gap)
            current = current.at[leading].add(own_term)
            return current.at[partner].add(back_term)

        def unchanged(current):
            return current

        return lax.cond(is_live, add_pair, unchanged, accum), None

    start_value = jnp.zeros(orbitals.shape, jnp.float32)
    exchange, unused = lax.scan(visit_pair, start_value, (flat_pairs, live_mask))
    return exchange
```

```python
import functools

import jax
import jax.numpy as jnp
from jax import lax
from jax.experimental import pallas as pl
from jax.experimental.pallas import tpu as pltpu
from jax.sharding import PartitionSpec as P

OWN, PEER, CROSS, RELAY, SWAP = range(5)
SWEEPS = 12
SPLIT = 2
LEAD = 8


def region_of(offset, core, chip_odd):
    near = jnp.where(core == 0, 1, -1)
    cross = jnp.where(chip_odd == 0, 2, -2)
    return jnp.where(
        offset == 0, OWN,
        jnp.where(offset == near, PEER,
                  jnp.where(offset == cross, CROSS,
                            jnp.where(offset == -cross, RELAY, SWAP))))


def solve_kernel(stage, counts, slots, orb_dev, margin, *refs):
    me_ref, rows_ref, offs_ref = refs[:3]
    at = 3
    regions = []
    for n in counts:
        regions.append(refs[at:at + n])
        at += n
    acc_ref = None
    if stage > 1:
        acc_ref = refs[at]
        at += 1
    out_ref, lead_buf, far_buf, part_buf, back_buf, b0, b1, b2, sems = refs[at:]
    nx, ny, nz = lead_buf.shape
    me = me_ref[0]
    core = lax.rem(me, 2)
    chip_odd = lax.rem(me // 2, 2)
    lanes = lax.broadcasted_iota(jnp.int32, (ny, nz), 1)
    first_lane, last_lane = lanes == 0, lanes == nz - 1
    inner = slice(LEAD, LEAD + ny)

    def start_up(x, _):
        for s in range(orb_dev):
            if acc_ref is None:
                out_ref[s, x] = jnp.zeros((ny, nz), jnp.float32)
            else:
                out_ref[s, x] = acc_ref[s, x]
        for buf in (far_buf, back_buf):
            buf[x, 0:margin] = jnp.zeros((margin, nz), jnp.float32)
            buf[x, margin + ny:] = jnp.zeros((margin, nz), jnp.float32)
        for buf in (b0, b1, b2):
            buf[x + 1, 0:LEAD] = jnp.zeros((LEAD, nz), jnp.float32)
            buf[x + 1, LEAD + ny:] = jnp.zeros((LEAD, nz), jnp.float32)
        return 0

    lax.fori_loop(0, nx, start_up, 0)
    for buf in (b0, b1, b2):
        buf[0] = jnp.zeros(buf.shape[1:], jnp.float32)
        buf[nx + 1] = jnp.zeros(buf.shape[1:], jnp.float32)

    def fetch(region, slot, place, sem):
        for code, pieces in enumerate(regions):
            for s in range(orb_dev):
                @pl.when((region == code) & (slot == s))
                def _():
                    if code == OWN:
                        pltpu.make_async_copy(pieces[0].at[s], place(0, nx), sem).start()
                    else:
                        each = len(pieces) // orb_dev
                        step = nx // each
                        for h in range(each):
                            pltpu.make_async_copy(
                                pieces[s * each + h].at[0], place(h * step, step), sem).start()

    def lead_place(x, n):
        return lead_buf.at[pl.ds(x, n)]

    def far_place(x, n):
        return far_buf.at[pl.ds(x, n), pl.ds(margin, ny)]

    def shifted_plane(buf, x, sx, sy, sz, keep):
        src = x - sx
        inside = (src >= 0) & (src < nx)
        plane = buf[jnp.clip(src, 0, nx - 1), pl.ds(margin - sy, ny), :]
        plane = pltpu.roll(plane, lax.rem(sz + nz, nz), axis=1)
        return jnp.where(keep & inside, plane, 0.0)

    def lanes_kept(sz):
        return (lanes >= sz) & (lanes < nz + sz)

    def stencil(src, write):
        def plane(x, carry):
            behind, here = carry
            ahead = src[x + 2, inner]
            total = behind + ahead
            total = total + (src[x + 1, LEAD - 1:LEAD - 1 + ny] + src[x + 1, LEAD + 1:LEAD + 1 + ny])
            left = jnp.where(first_lane, 0.0, pltpu.roll(here, 1, axis=1))
            right = jnp.where(last_lane, 0.0, pltpu.roll(here, nz - 1, axis=1))
            write(x, here, total + (left + right))
            return here, ahead
        lax.fori_loop(0, nx, plane, (src[0, inner], src[1, inner]), unroll=2)

    def into(dst):
        def write(x, here, total):
            dst[x + 1, inner] = total
        return write

    def visit(k, _):
        r, t = k // slots, lax.rem(k, slots)
        lead = rows_ref[r, 1 + 2 * t]
        far = rows_ref[r, 2 + 2 * t]
        lead_off = lead // orb_dev - me
        far_off = far // orb_dev - me
        lead_region = region_of(lead_off, core, chip_odd)
        far_region = region_of(far_off, core, chip_odd)
        mine = (lead_off == 0) | (far_off == 0)
        top = jnp.maximum(lead_region, far_region)
        when = jnp.where(top <= PEER, 1, jnp.where(top == CROSS, 2, 3))

        @pl.when((t < rows_ref[r, 0]) & mine & (when == stage))
        def _():
            lead_slot = lax.rem(lead, orb_dev)
            far_slot = lax.rem(far, orb_dev)
            sx, sy, sz = [offs_ref[far * 3 + a] - offs_ref[lead * 3 + a] for a in range(3)]
            fetch(lead_region, lead_slot, lead_place, sems.at[0])
            fetch(far_region, far_slot, far_place, sems.at[1])
            pltpu.make_async_copy(regions[0][0].at[0], lead_place(0, nx), sems.at[0]).wait()
            pltpu.make_async_copy(regions[0][0].at[0], far_place(0, nx), sems.at[1]).wait()
            keep = lanes_kept(sz)

            def build(x, _):
                partner = shifted_plane(far_buf, x, sx, sy, sz, keep)
                part_buf[x] = partner
                b0[x + 1, inner] = lead_buf[x] * partner
                return 0

            lax.fori_loop(0, nx, build, 0, unroll=2)

            stencil(b0, into(b1))

            def first(x, here, total):
                b2[x + 1, inner] = 36.0 * b0[x + 1, inner] + (6.0 * here + total)
            stencil(b1, first)
            stencil(b2, into(b0))
            stencil(b0, into(b1))

            def second(x, here, total):
                b0[x + 1, inner] = 216.0 * b2[x + 1, inner] + total
            stencil(b1, second)
            stencil(b0, into(b1))
            stencil(b1, into(b2))
            stencil(b2, into(b1))
            stencil(b1, into(b2))
            stencil(b2, into(b1))

            def third(x, here, total):
                b2[x + 1, inner] = (6.0 ** 6 * b0[x + 1, inner] + total) * (6.0 ** -12)
            stencil(b1, third)

            @pl.when(lead_off == 0)
            def _():
                def add(x, _):
                    out_ref[lead_slot, x] += b2[x + 1, inner] * part_buf[x]
                    return 0
                lax.fori_loop(0, nx, add, 0, unroll=2)

            @pl.when(far_off == 0)
            def _():
                def product(x, _):
                    back_buf[x, pl.ds(margin, ny)] = b2[x + 1, inner] * lead_buf[x]
                    return 0
                lax.fori_loop(0, nx, product, 0, unroll=2)
                back_keep = lanes_kept(-sz)

                def add(x, _):
                    out_ref[far_slot, x] += shifted_plane(back_buf, x, -sx, -sy, -sz, back_keep)
                    return 0
                lax.fori_loop(0, nx, add, 0, unroll=2)
        return 0

    lax.fori_loop(0, 3 * slots, visit, 0)


def solve(stage, me, rows, offs, regions, acc, shape):
    orb_dev, nx, ny, nz = shape
    margin = nx // 2
    slots = (rows.shape[1] - 1) // 2
    counts = [len(r) for r in regions]
    flat = [piece for r in regions for piece in r]
    smem = pl.BlockSpec(memory_space=pltpu.SMEM)
    vmem = pl.BlockSpec(memory_space=pltpu.VMEM)
    in_specs = [smem] * 3 + [pl.BlockSpec(memory_space=pl.ANY)] * len(flat)
    args = [me, rows, offs] + flat
    aliases = {}
    if acc is not None:
        aliases = {len(args): 0}
        in_specs.append(vmem)
        args.append(acc)
    padded = (nx, ny + 2 * margin, nz)
    work = (nx + 2, ny + 2 * LEAD, nz)
    return pl.pallas_call(
        functools.partial(solve_kernel, stage, counts, slots, orb_dev, margin),
        out_shape=jax.ShapeDtypeStruct(shape, jnp.float32),
        in_specs=in_specs,
        out_specs=vmem,
        scratch_shapes=[
            pltpu.VMEM((nx, ny, nz), jnp.float32),
            pltpu.VMEM(padded, jnp.float32),
            pltpu.VMEM((nx, ny, nz), jnp.float32),
            pltpu.VMEM(padded, jnp.float32),
            pltpu.VMEM(work, jnp.float32),
            pltpu.VMEM(work, jnp.float32),
            pltpu.VMEM(work, jnp.float32),
            pltpu.SemaphoreType.DMA((2,)),
        ],
        input_output_aliases=aliases,
        compiler_params=pltpu.CompilerParams(vmem_limit_bytes=58 << 20),
        cost_estimate=pl.CostEstimate(flops=40_000_000, bytes_accessed=60_000_000, transcendentals=0),
        name=f"solve{stage}",
    )(*args)


def local(size, orbitals, pair_list, pair_count, box_offset):
    shape = orbitals.shape
    orb_dev, nx = shape[:2]
    me = lax.axis_index("orb").astype(jnp.int32)
    core, chip_odd = me % 2, (me // 2) % 2

    def send(value, route):
        moves = [(s, route(s)) for s in range(size)]
        return lax.ppermute(value, "orb", [m for m in moves if 0 <= m[1] < size])

    def to_peer(s):
        return s ^ 1

    def to_pair(s):
        return s ^ 2

    def onward(s):
        return s + 4 if (s // 2) % 2 == 0 else s - 4

    row = jnp.concatenate([pair_count[:, None], pair_list.reshape(1, -1)], 1)
    rows = jnp.concatenate(
        [send(row, lambda s: s + 1), row, send(row, lambda s: s - 1)], 0)
    step = nx // SPLIT
    pieces = [orbitals[o:o + 1, h * step:(h + 1) * step] for o in range(orb_dev) for h in range(SPLIT)]
    peer = [send(p, to_peer) for p in pieces]
    cross = [send(p, to_pair) for p in pieces]
    common = (me[None], rows, box_offset.reshape(-1))
    acc = solve(1, *common, [[orbitals], peer], None, shape)
    done = acc[0, 0, 0, :1]
    relay = [send(lax.optimization_barrier((p, done))[0], onward) for p in cross]
    give_cross = core == chip_odd
    swap = [send(jnp.where(give_cross, c, r), to_peer) for c, r in zip(cross, relay)]
    acc = solve(2, *common, [[orbitals], peer, cross], acc, shape)
    return solve(3, *common, [[orbitals], peer, cross, relay, swap], acc, shape)


def solution(mesh):
    placed = (P("orb", None, None, None), P("orb", None, None), P("orb"), P())
    return jax.shard_map(
        functools.partial(local, mesh.shape["orb"]), mesh=mesh, in_specs=placed,
        out_specs=P("orb", None, None, None), check_vma=False)
```

```python
import functools

import jax
import jax.numpy as jnp
import numpy as np
from jax import lax
from jax.experimental import pallas as pl
from jax.experimental.pallas import tpu as pltpu
from jax.sharding import PartitionSpec as P

OWN, PEER, CROSS, RELAY, SWAP = range(5)
SWEEPS = 12
SPLIT = 2
CHUNK = 8


def region_of(offset, core, chip_odd):
    near = jnp.where(core == 0, 1, -1)
    cross = jnp.where(chip_odd == 0, 2, -2)
    return jnp.where(
        offset == 0, OWN,
        jnp.where(offset == near, PEER,
                  jnp.where(offset == cross, CROSS,
                            jnp.where(offset == -cross, RELAY, SWAP))))


def solve_kernel(stage, counts, slots, orb_dev, margin, *refs):
    me_ref, rows_ref, offs_ref, z_hi_ref, z_lo_ref, y_ref, eig_ref = refs[:7]
    at = 7
    regions = []
    for n in counts:
        regions.append(refs[at:at + n])
        at += n
    acc_ref = None
    if stage > 1:
        acc_ref = refs[at]
        at += 1
    out_ref, lead_buf, far_buf, part_buf, back_buf, b0, sems = refs[at:]
    nx, ny, nz = lead_buf.shape
    me = me_ref[0]
    core = lax.rem(me, 2)
    chip_odd = lax.rem(me // 2, 2)
    lanes = lax.broadcasted_iota(jnp.int32, (ny, nz), 1)

    def start_up(x, _):
        for s in range(orb_dev):
            if acc_ref is None:
                out_ref[s, x] = jnp.zeros((ny, nz), jnp.float32)
            else:
                out_ref[s, x] = acc_ref[s, x]
        for buf in (far_buf, back_buf):
            buf[x, 0:margin] = jnp.zeros((margin, nz), jnp.float32)
            buf[x, margin + ny:] = jnp.zeros((margin, nz), jnp.float32)
        return 0

    lax.fori_loop(0, nx, start_up, 0, unroll=4)

    def fetch(region, slot, place, sem):
        for code, pieces in enumerate(regions):
            for s in range(orb_dev):
                @pl.when((region == code) & (slot == s))
                def _():
                    if code == OWN:
                        pltpu.make_async_copy(pieces[0].at[s], place(0, nx), sem).start()
                    else:
                        each = len(pieces) // orb_dev
                        step = nx // each
                        for h in range(each):
                            pltpu.make_async_copy(
                                pieces[s * each + h].at[0], place(h * step, step), sem).start()

    def lead_place(x, n):
        return lead_buf.at[pl.ds(x, n)]

    def far_place(x, n):
        return far_buf.at[pl.ds(x, n), pl.ds(margin, ny)]

    def shifted_plane(buf, x, sx, sy, sz, keep):
        src = x - sx
        inside = (src >= 0) & (src < nx)
        plane = buf[jnp.clip(src, 0, nx - 1), pl.ds(margin - sy, ny), :]
        plane = pltpu.roll(plane, lax.rem(sz + nz, nz), axis=1)
        return jnp.where(keep & inside, plane, 0.0)

    def lanes_kept(sz):
        return (lanes >= sz) & (lanes < nz + sz)

    mats = dict(zip(("z_hi", "z_lo", "y"), (z_hi_ref, z_lo_ref, y_ref)))

    def split(v):
        hi = v.astype(jnp.bfloat16)
        return hi, (v - hi.astype(jnp.float32)).astype(jnp.bfloat16)

    def along_z(v):
        hi, lo = split(v.reshape(-1, nz))
        out = jnp.dot(jnp.concatenate([hi, lo], 1), mats["z_hi"][...], preferred_element_type=jnp.float32)
        out = out + jnp.dot(hi, mats["z_lo"][...], preferred_element_type=jnp.float32)
        return out.reshape(v.shape)

    def along_y(v):
        planes = []
        for n in range(0, v.shape[0], 2):
            hi, lo = split(jnp.concatenate([v[n], v[n + 1]], 1))
            out = jnp.dot(mats["y"][...], jnp.concatenate([hi, lo, hi], 0), preferred_element_type=jnp.float32)
            planes += [out[:, :nz], out[:, nz:]]
        return jnp.stack(planes)

    def along_x(t, _):
        y0 = pl.multiple_of(t * 8, 8)
        eigen = eig_ref[pl.ds(y0, 8), :]

        def apply(v):
            out = []
            for x in range(nx):
                term = eigen * v[x]
                if 0 < x < nx - 1:
                    term = term + (v[x - 1] + v[x + 1])
                else:
                    term = term + (v[1] if x == 0 else v[nx - 2])
                out.append(term)
            return out

        d = [b0[x, pl.ds(y0, 8)] for x in range(nx)]
        one = apply(d)
        two = apply(one)
        v = [36.0 * p + (6.0 * q + r) for p, q, r in zip(d, one, two)]
        w = v
        for _ in range(3):
            w = apply(w)
        v = [216.0 * p + q for p, q in zip(v, w)]
        w = v
        for _ in range(6):
            w = apply(w)
        for x in range(nx):
            b0[x, pl.ds(y0, 8)] = (6.0 ** 6 * v[x] + w[x]) * (6.0 ** -12)
        return 0

    def visit(k, _):
        r, t = k // slots, lax.rem(k, slots)
        lead = rows_ref[r, 1 + 2 * t]
        far = rows_ref[r, 2 + 2 * t]
        lead_off = lead // orb_dev - me
        far_off = far // orb_dev - me
        lead_region = region_of(lead_off, core, chip_odd)
        far_region = region_of(far_off, core, chip_odd)
        mine = (lead_off == 0) | (far_off == 0)
        top = jnp.maximum(lead_region, far_region)
        when = jnp.where(top <= PEER, 1, jnp.where(top == CROSS, 2, 3))

        @pl.when((t < rows_ref[r, 0]) & mine & (when == stage))
        def _():
            lead_slot = lax.rem(lead, orb_dev)
            far_slot = lax.rem(far, orb_dev)
            sx, sy, sz = [offs_ref[far * 3 + a] - offs_ref[lead * 3 + a] for a in range(3)]
            fetch(lead_region, lead_slot, lead_place, sems.at[0])
            fetch(far_region, far_slot, far_place, sems.at[1])
            pltpu.make_async_copy(regions[0][0].at[0], lead_place(0, nx), sems.at[0]).wait()
            pltpu.make_async_copy(regions[0][0].at[0], far_place(0, nx), sems.at[1]).wait()
            keep = lanes_kept(sz)

            def forward(c, _):
                x0 = c * CHUNK
                dens = []
                for h in range(CHUNK):
                    partner = shifted_plane(far_buf, x0 + h, sx, sy, sz, keep)
                    part_buf[x0 + h] = partner
                    dens.append(lead_buf[x0 + h] * partner)
                b0[pl.ds(x0, CHUNK)] = along_y(along_z(jnp.stack(dens)))
                return 0

            lax.fori_loop(0, nx // CHUNK, forward, 0)
            lax.fori_loop(0, ny // 8, along_x, 0)

            def backward(c, _):
                at_x = pl.ds(c * CHUNK, CHUNK)
                b0[at_x] = along_z(along_y(b0[at_x]))
                return 0

            lax.fori_loop(0, nx // CHUNK, backward, 0)

            @pl.when(lead_off == 0)
            def _():
                def add(c, _):
                    at_x = pl.ds(c * CHUNK, CHUNK)
                    out_ref[lead_slot, at_x] += b0[at_x] * part_buf[at_x]
                    return 0
                lax.fori_loop(0, nx // CHUNK, add, 0)

            @pl.when(far_off == 0)
            def _():
                def product(c, _):
                    at_x = pl.ds(c * CHUNK, CHUNK)
                    back_buf[at_x, pl.ds(margin, ny)] = b0[at_x] * lead_buf[at_x]
                    return 0
                lax.fori_loop(0, nx // CHUNK, product, 0)
                back_keep = lanes_kept(-sz)

                def add(c, _):
                    for h in range(CHUNK):
                        x = c * CHUNK + h
                        out_ref[far_slot, x] += shifted_plane(back_buf, x, -sx, -sy, -sz, back_keep)
                    return 0
                lax.fori_loop(0, nx // CHUNK, add, 0)
        return 0

    lax.fori_loop(0, 3 * slots, visit, 0)


def sine_tables(ny, nz):
    def table(n):
        grid = np.outer(np.arange(1, n + 1), np.arange(1, n + 1))
        return np.sqrt(2 / (n + 1)) * np.sin(np.pi * grid / (n + 1))

    def eigen(n):
        return 2 * np.cos(np.pi * np.arange(1, n + 1) / (n + 1))

    def halves(m):
        hi = m.astype(jnp.bfloat16)
        return hi, (m - hi.astype(np.float64)).astype(jnp.bfloat16)

    z_hi, z_lo = halves(table(nz))
    y_hi, y_lo = halves(table(ny))
    tables = (np.concatenate([z_hi, z_hi], 0), z_lo, np.concatenate([y_hi, y_hi, y_lo], 1))
    return [jnp.asarray(t) for t in tables] + [
        jnp.asarray((eigen(ny)[:, None] + eigen(nz)[None, :]).astype(np.float32))]


def solve(stage, me, rows, offs, regions, acc, shape):
    orb_dev, nx, ny, nz = shape
    margin = nx // 2
    slots = (rows.shape[1] - 1) // 2
    counts = [len(r) for r in regions]
    flat = [piece for r in regions for piece in r]
    smem = pl.BlockSpec(memory_space=pltpu.SMEM)
    vmem = pl.BlockSpec(memory_space=pltpu.VMEM)
    tables = sine_tables(ny, nz)
    in_specs = [smem] * 3 + [vmem] * len(tables) + [pl.BlockSpec(memory_space=pl.ANY)] * len(flat)
    args = [me, rows, offs, *tables] + flat
    aliases = {}
    if acc is not None:
        aliases = {len(args): 0}
        in_specs.append(vmem)
        args.append(acc)
    padded = (nx, ny + 2 * margin, nz)
    return pl.pallas_call(
        functools.partial(solve_kernel, stage, counts, slots, orb_dev, margin),
        out_shape=jax.ShapeDtypeStruct(shape, jnp.float32),
        in_specs=in_specs,
        out_specs=vmem,
        scratch_shapes=[
            pltpu.VMEM((nx, ny, nz), jnp.float32),
            pltpu.VMEM(padded, jnp.float32),
            pltpu.VMEM((nx, ny, nz), jnp.float32),
            pltpu.VMEM(padded, jnp.float32),
            pltpu.VMEM((nx, ny, nz), jnp.float32),
            pltpu.SemaphoreType.DMA((2,)),
        ],
        input_output_aliases=aliases,
        compiler_params=pltpu.CompilerParams(vmem_limit_bytes=58 << 20),
        cost_estimate=pl.CostEstimate(flops=40_000_000, bytes_accessed=60_000_000, transcendentals=0),
        name=f"solve{stage}",
    )(*args)


def local(size, orbitals, pair_list, pair_count, box_offset):
    shape = orbitals.shape
    orb_dev, nx = shape[:2]
    me = lax.axis_index("orb").astype(jnp.int32)
    core, chip_odd = me % 2, (me // 2) % 2

    def send(value, route):
        moves = [(s, route(s)) for s in range(size)]
        return lax.ppermute(value, "orb", [m for m in moves if 0 <= m[1] < size])

    def to_peer(s):
        return s ^ 1

    def to_pair(s):
        return s ^ 2

    def onward(s):
        return s + 4 if (s // 2) % 2 == 0 else s - 4

    row = jnp.concatenate([pair_count[:, None], pair_list.reshape(1, -1)], 1)
    rows = jnp.concatenate(
        [send(row, lambda s: s + 1), row, send(row, lambda s: s - 1)], 0)
    step = nx // SPLIT
    pieces = [orbitals[o:o + 1, h * step:(h + 1) * step] for o in range(orb_dev) for h in range(SPLIT)]
    peer = [send(p, to_peer) for p in pieces]
    cross = [send(lax.optimization_barrier((p, rows))[0], to_pair) for p in pieces]
    def after(acc, values):
        mark = acc[0, 0, 0, :1]
        return [lax.optimization_barrier((v, mark))[0] for v in values]

    common = (me[None], rows, box_offset.reshape(-1))
    acc = solve(1, *common, [[orbitals], peer], None, shape)
    relay = [send(p, onward) for p in after(acc, cross)]
    acc = solve(2, *common, [[orbitals], peer, cross], acc, shape)
    give_cross = core == chip_odd
    swap = [send(jnp.where(give_cross, c, r), to_peer) for c, r in zip(cross, after(acc, relay))]
    return solve(3, *common, [[orbitals], peer, cross, relay, swap], acc, shape)


def solution(mesh):
    placed = (P("orb", None, None, None), P("orb", None, None), P("orb"), P())
    return jax.shard_map(
        functools.partial(local, mesh.shape["orb"]), mesh=mesh, in_specs=placed,
        out_specs=P("orb", None, None, None), check_vma=False)
```

```python
import functools

import jax
import jax.numpy as jnp
import numpy as np
from jax import lax
from jax.experimental import pallas as pl
from jax.experimental.pallas import tpu as pltpu
from jax.sharding import PartitionSpec as P


OWN, PEER, CROSS, RELAY, SWAP = range(5)
SPLIT = 2
NEAR_STOPS = (1, 3, 5, 7)
CHUNK = 8


def region_of(offset, core, chip_odd):
    near = jnp.where(core == 0, 1, -1)
    cross = jnp.where(chip_odd == 0, 2, -2)
    return jnp.where(
        offset == 0, OWN,
        jnp.where(offset == near, PEER,
                  jnp.where(offset == cross, CROSS,
                            jnp.where(offset == -cross, RELAY, SWAP))))


def solve_kernel(stage, first, ranks, counts, slots, orb_dev, margin, *refs):
    me_ref, rows_ref, offs_ref, z_hi_ref, z_lo_ref, y_ref, eig_ref = refs[:7]
    at = 7
    regions = []
    for n in counts:
        regions.append(refs[at:at + n])
        at += n
    if not first:
        at += 1
    result_ref, lead_buf, far_buf, part_buf, back_buf, b0, out_ref, sems, loaded = refs[at:]
    nx, ny, nz = lead_buf.shape
    me = me_ref[0]
    core = lax.rem(me, 2)
    chip_odd = lax.rem(me // 2, 2)
    lanes = lax.broadcasted_iota(jnp.int32, (ny, nz), 1)

    def start_up():
        def one(x, _):
            for buf in (far_buf, back_buf):
                buf[x, 0:margin] = jnp.zeros((margin, nz), jnp.float32)
                buf[x, margin + ny:] = jnp.zeros((margin, nz), jnp.float32)
            if first:
                for s in range(orb_dev):
                    out_ref[s, x] = jnp.zeros((ny, nz), jnp.float32)
            return 0

        if not first:
            load = pltpu.make_async_copy(result_ref, out_ref, sems.at[2])
            load.start()
        lax.fori_loop(0, nx, one, 0, unroll=4)
        if not first:
            load.wait()
        loaded[0] = 1

    loaded[0] = 0
    if first:
        start_up()

    def fetch(region, slot, place, sem):
        for code, pieces in enumerate(regions):
            for s in range(orb_dev):
                @pl.when((region == code) & (slot == s))
                def _():
                    if code == OWN:
                        pltpu.make_async_copy(pieces[0].at[s], place(0, nx), sem).start()
                    else:
                        each = len(pieces) // orb_dev
                        step = nx // each
                        for h in range(each):
                            pltpu.make_async_copy(
                                pieces[s * each + h].at[0], place(h * step, step), sem).start()

    def lead_place(x, n):
        return lead_buf.at[pl.ds(x, n)]

    def far_place(x, n):
        return far_buf.at[pl.ds(x, n), pl.ds(margin, ny)]

    def shifted_plane(buf, x, sx, sy, sz, keep):
        src = x - sx
        inside = (src >= 0) & (src < nx)
        plane = buf[jnp.clip(src, 0, nx - 1), pl.ds(margin - sy, ny), :]
        plane = pltpu.roll(plane, lax.rem(sz + nz, nz), axis=1)
        return jnp.where(keep & inside, plane, 0.0)

    def lanes_kept(sz):
        return (lanes >= sz) & (lanes < nz + sz)

    mats = dict(zip(("z_hi", "z_lo", "y"), (z_hi_ref, z_lo_ref, y_ref)))

    def split(v):
        hi = v.astype(jnp.bfloat16)
        return hi, (v - hi.astype(jnp.float32)).astype(jnp.bfloat16)

    def along_z(v):
        hi, lo = split(v.reshape(-1, nz))
        out = jnp.dot(jnp.concatenate([hi, lo], 1), mats["z_hi"][...], preferred_element_type=jnp.float32)
        out = out + jnp.dot(hi, mats["z_lo"][...], preferred_element_type=jnp.float32)
        return out.reshape(v.shape)

    def along_y(v):
        planes = []
        for n in range(0, v.shape[0], 2):
            hi, lo = split(jnp.concatenate([v[n], v[n + 1]], 1))
            out = jnp.dot(mats["y"][...], jnp.concatenate([hi, lo, hi], 0), preferred_element_type=jnp.float32)
            planes += [out[:, :nz], out[:, nz:]]
        return jnp.stack(planes)

    def along_x(t, _):
        y0 = pl.multiple_of(t * 8, 8)
        eigen = eig_ref[pl.ds(y0, 8), :]

        def apply(v):
            out = []
            for x in range(nx):
                term = eigen * v[x]
                if 0 < x < nx - 1:
                    term = term + (v[x - 1] + v[x + 1])
                else:
                    term = term + (v[1] if x == 0 else v[nx - 2])
                out.append(term)
            return out

        d = [b0[x, pl.ds(y0, 8)] for x in range(nx)]
        one = apply(d)
        two = apply(one)
        v = [36.0 * p + (6.0 * q + r) for p, q, r in zip(d, one, two)]
        w = v
        for _ in range(3):
            w = apply(w)
        v = [216.0 * p + q for p, q in zip(v, w)]
        w = v
        for _ in range(6):
            w = apply(w)
        for x in range(nx):
            b0[x, pl.ds(y0, 8)] = (6.0 ** 6 * v[x] + w[x]) * (6.0 ** -12)
        return 0

    def visit(k, seen):
        r, t = k // slots, lax.rem(k, slots)
        lead = rows_ref[r, 1 + 2 * t]
        far = rows_ref[r, 2 + 2 * t]
        lead_off = lead // orb_dev - me
        far_off = far // orb_dev - me
        lead_region = region_of(lead_off, core, chip_odd)
        far_region = region_of(far_off, core, chip_odd)
        mine = (lead_off == 0) | (far_off == 0)
        top = jnp.maximum(lead_region, far_region)
        when = jnp.where(top <= PEER, 1, jnp.where(top == CROSS, 2, 3))

        live = (t < rows_ref[r, 0]) & mine
        near = live & (when == 1)
        now = near & (seen >= ranks[0]) & (seen < ranks[1])
        if stage > 1:
            now = now | (live & (when == stage))

        @pl.when(now)
        def _():
            if not first:
                pl.when(loaded[0] == 0)(start_up)
            lead_slot = lax.rem(lead, orb_dev)
            far_slot = lax.rem(far, orb_dev)
            sx, sy, sz = [offs_ref[far * 3 + a] - offs_ref[lead * 3 + a] for a in range(3)]
            fetch(lead_region, lead_slot, lead_place, sems.at[0])
            fetch(far_region, far_slot, far_place, sems.at[1])
            pltpu.make_async_copy(regions[0][0].at[0], lead_place(0, nx), sems.at[0]).wait()
            pltpu.make_async_copy(regions[0][0].at[0], far_place(0, nx), sems.at[1]).wait()
            keep = lanes_kept(sz)

            def forward(c, _):
                x0 = c * CHUNK
                dens = []
                for h in range(CHUNK):
                    partner = shifted_plane(far_buf, x0 + h, sx, sy, sz, keep)
                    part_buf[x0 + h] = partner
                    dens.append(lead_buf[x0 + h] * partner)
                b0[pl.ds(x0, CHUNK)] = along_y(along_z(jnp.stack(dens)))
                return 0

            lax.fori_loop(0, nx // CHUNK, forward, 0)
            lax.fori_loop(0, ny // 8, along_x, 0)

            def backward(c, _):
                at_x = pl.ds(c * CHUNK, CHUNK)
                b0[at_x] = along_z(along_y(b0[at_x]))
                return 0

            lax.fori_loop(0, nx // CHUNK, backward, 0)

            @pl.when(lead_off == 0)
            def _():
                def add(c, _):
                    at_x = pl.ds(c * CHUNK, CHUNK)
                    out_ref[lead_slot, at_x] += b0[at_x] * part_buf[at_x]
                    return 0

                lax.fori_loop(0, nx // CHUNK, add, 0)

            @pl.when(far_off == 0)
            def _():
                def product(c, _):
                    at_x = pl.ds(c * CHUNK, CHUNK)
                    back_buf[at_x, pl.ds(margin, ny)] = b0[at_x] * lead_buf[at_x]
                    return 0

                lax.fori_loop(0, nx // CHUNK, product, 0)
                back_keep = lanes_kept(-sz)

                def add(c, _):
                    for h in range(CHUNK):
                        x = c * CHUNK + h
                        out_ref[far_slot, x] += shifted_plane(back_buf, x, -sx, -sy, -sz, back_keep)
                    return 0

                lax.fori_loop(0, nx // CHUNK, add, 0)

        return seen + near.astype(jnp.int32)

    lax.fori_loop(0, 3 * slots, visit, jnp.int32(0))

    @pl.when(loaded[0] == 1)
    def _():
        store = pltpu.make_async_copy(out_ref, result_ref, sems.at[2])
        store.start()
        store.wait()


def sine_tables(ny, nz):
    def table(n):
        grid = np.outer(np.arange(1, n + 1), np.arange(1, n + 1))
        return np.sqrt(2 / (n + 1)) * np.sin(np.pi * grid / (n + 1))

    def eigen(n):
        return 2 * np.cos(np.pi * np.arange(1, n + 1) / (n + 1))

    def halves(m):
        hi = m.astype(jnp.bfloat16)
        return hi, (m - hi.astype(np.float64)).astype(jnp.bfloat16)

    z_hi, z_lo = halves(table(nz))
    y_hi, y_lo = halves(table(ny))
    tables = (np.concatenate([z_hi, z_hi], 0), z_lo, np.concatenate([y_hi, y_hi, y_lo], 1))
    return [jnp.asarray(t) for t in tables] + [
        jnp.asarray((eigen(ny)[:, None] + eigen(nz)[None, :]).astype(np.float32))]


def solve(stage, ranks, me, rows, offs, regions, acc, shape):
    orb_dev, nx, ny, nz = shape
    margin = nx // 2
    slots = (rows.shape[1] - 1) // 2
    counts = [len(r) for r in regions]
    flat = [piece for r in regions for piece in r]
    smem = pl.BlockSpec(memory_space=pltpu.SMEM)
    vmem = pl.BlockSpec(memory_space=pltpu.VMEM)
    tables = sine_tables(ny, nz)
    in_specs = [smem] * 3 + [vmem] * len(tables) + [pl.BlockSpec(memory_space=pl.ANY)] * len(flat)
    args = [me, rows, offs, *tables] + flat
    aliases = {}
    if acc is not None:
        aliases = {len(args): 0}
        in_specs.append(pl.BlockSpec(memory_space=pl.ANY))
        args.append(acc)
    padded = (nx, ny + 2 * margin, nz)
    return pl.pallas_call(
        functools.partial(solve_kernel, stage, acc is None, ranks, counts, slots, orb_dev, margin),
        out_shape=jax.ShapeDtypeStruct(shape, jnp.float32),
        in_specs=in_specs,
        out_specs=pl.BlockSpec(memory_space=pl.ANY),
        scratch_shapes=[
            pltpu.VMEM((nx, ny, nz), jnp.float32),
            pltpu.VMEM(padded, jnp.float32),
            pltpu.VMEM((nx, ny, nz), jnp.float32),
            pltpu.VMEM(padded, jnp.float32),
            pltpu.VMEM((nx, ny, nz), jnp.float32),
            pltpu.VMEM(shape, jnp.float32),
            pltpu.SemaphoreType.DMA((3,)),
            pltpu.SMEM((1,), jnp.int32),
        ],
        input_output_aliases=aliases,
        compiler_params=pltpu.CompilerParams(vmem_limit_bytes=58 << 20),
        cost_estimate=pl.CostEstimate(flops=40_000_000, bytes_accessed=60_000_000, transcendentals=0),
    )(*args)


def local(size, orbitals, pair_list, pair_count, box_offset):
    shape = orbitals.shape
    orb_dev, nx = shape[:2]
    me = lax.axis_index("orb").astype(jnp.int32)
    core, chip_odd = me % 2, (me // 2) % 2

    def send(value, route):
        moves = [(s, route(s)) for s in range(size)]
        return lax.ppermute(value, "orb", [m for m in moves if 0 <= m[1] < size])

    def to_peer(s):
        return s ^ 1

    def to_pair(s):
        return s ^ 2

    def onward(s):
        return s + 4 if (s // 2) % 2 == 0 else s - 4

    row = jnp.concatenate([pair_count[:, None], pair_list.reshape(1, -1)], 1)
    rows = jnp.concatenate(
        [send(row, lambda s: s + 1), row, send(row, lambda s: s - 1)], 0)
    step = nx // SPLIT
    pieces = [orbitals[o:o + 1, h * step:(h + 1) * step] for o in range(orb_dev) for h in range(SPLIT)]
    peer = [send(p, to_peer) for p in pieces]
    cross = [send(lax.optimization_barrier((p, rows))[0], to_pair) for p in pieces]
    common = (me[None], rows, box_offset.reshape(-1))
    acc, relay, start = None, [], 0
    for piece, stop in zip(cross, NEAR_STOPS):
        acc = solve(1, (start, stop), *common, [[orbitals], peer], acc, shape)
        start = stop
        relay.append(send(piece, onward))
    acc = solve(2, (start, start), *common, [[orbitals], peer, cross], acc, shape)
    give_cross = core == chip_odd
    swap = []
    for c, r in zip(cross, relay):
        swap.append(send(jnp.where(give_cross, c, r), to_peer))
    everything = [[orbitals], peer, cross, relay, swap]
    return solve(3, (start, rows.shape[0] * rows.shape[1]), *common, everything, acc, shape)


def solution(mesh):
    placed = (P("orb", None, None, None), P("orb", None, None), P("orb"), P())

    def body(*args):
        return local(mesh.shape["orb"], *args)

    return jax.shard_map(
        body, mesh=mesh, in_specs=placed,
        out_specs=P("orb", None, None, None), check_vma=False)
```
